256 devices in a mesh: grp: 4 (over y_lo, core), sp: 64 (over y_hi, z, x).
Axes of the slice: x: 4, y: 4 (y_hi: 2, y_lo: 2; y = y_hi * 2 + y_lo), z: 8, core: 2. Of those that a mesh axis runs over, the one named last changes fastest.
Arguments:
- flame_state: float32 [54, 128, 512], P(None, 'sp', 'grp'), may hold values from -1 to 2, as said below
- tangents: float32 [12, 54, 128, 512], P('grp', None, 'sp'), may hold values from -6 to 6
- direction_index: int32 [12], P('grp'), may hold values from 0 to 324
- reactant_table: int32 [325, 53], replicated, may hold values from 0 to 2, as said below
- product_table: int32 [325, 53], replicated, may hold values from 0 to 2, as said below
- natural_log_frequency: float32 [325], replicated, may hold values from -3 to -1
- arrhenius_energy: float32 [325], replicated, may hold values from 0.5 to 3
- diffusivity: float32 [54], replicated, may hold values from 0.03 to 0.25
- enthalpy: float32 [53], replicated, may hold values from -0.5 to 0.5
Outputs:
- new_state: float32 [54, 128, 512], P(None, 'sp', 'grp')
- new_tangents: float32 [12, 54, 128, 512], P('grp', None, 'sp')
The draws below stay inside these ranges and needn't reach their ends.
Inputs may be any that keep to these rules, and one draw needn't show every extreme that they name: `flame_state`: rows 0 to 52 are log concentrations in [-1, 0.5]; the last row is temperature in [1, 2]. `reactant_table`: each reaction has one or two reactant units; a species may count twice. `product_table`: each reaction has one or two product units; a species may count twice.
All inputs are finite; a program needn't handle non-finite values.
Results may differ from the reference program's by a relative error of at most 0.0003.
Values sent between devices are 32-bit elements; how exact they have to be, the bound alone decides.
No kernel may reach another device: no remote copies, remote signals or barrier semaphores. Data moves between devices by JAX's collectives and lax.ppermute only.
A program may use at most 128 MiB of HBM per device.

```python
import math
import jax
import jax.numpy as jnp
from jax import lax

SPECIES = 53
REACTIONS = 325
FIELDS = 54
GRID_POINTS_TWO = 16
GRID_POINTS_THREE = 32
CELLS = 512
GRID_POINTS_ONE = 128
DIRECTIONS = 12


def draw_flame_state(key, part):
    component_seed_handle, thermal_seed_handle = jax.random.split(key)
    exponent_numbers = jax.random.uniform(component_seed_handle, (SPECIES, GRID_POINTS_ONE, GRID_POINTS_TWO * GRID_POINTS_THREE), jnp.float32, -1.0, 0.5)
    mixture_heat_level = jax.random.uniform(thermal_seed_handle, (1, GRID_POINTS_ONE, GRID_POINTS_TWO * GRID_POINTS_THREE), jnp.float32, 1.0, 2.0)
    return jnp.concatenate([exponent_numbers, mixture_heat_level], 0)


def stoich(key):
    leading_key, partner_key, doubled_key = jax.random.split(key, 3)
    leading = jax.random.randint(leading_key, (REACTIONS,), 0, SPECIES)
    partner = jax.random.randint(partner_key, (REACTIONS,), 0, SPECIES)
    doubled = jax.random.randint(doubled_key, (REACTIONS,), 0, 2)
    reaction_ids = jnp.arange(REACTIONS, dtype=jnp.int32)
    partner = jnp.where(reaction_ids == 0, leading, partner)
    doubled = jnp.where(reaction_ids == 0, 1, doubled)
    species_ids = jnp.arange(SPECIES, dtype=jnp.int32)
    single = (leading[:, None] == species_ids[None, :]).astype(jnp.int32)
    second_unit = (partner[:, None] == species_ids[None, :]).astype(jnp.int32)
    return single + doubled[:, None] * second_unit


def draw_reactant_table(key, part):
    return stoich(jax.random.fold_in(key, 11))


def draw_product_table(key, part):
    return stoich(jax.random.fold_in(key, 23))


def touch_ends(drawn, stream_key, low, high):
    longest = drawn.shape.index(max(drawn.shape))
    spots = []
    for shift in (0, 1):
        where = [jax.random.randint(jax.random.fold_in(stream_key, axis), (), 0, length) for axis, length in enumerate(drawn.shape)]
        where[longest] = (where[longest] + shift) % drawn.shape[longest]
        spots.append(tuple(where))
    return drawn.at[spots[0]].set(low).at[spots[1]].set(high)


def levels(rng, dims, cuts, low, largest):
    level = 1.0
    for dim, shards_of in cuts:
        steps = jax.random.uniform(jax.random.fold_in(jax.random.fold_in(rng, 6), dim), (shards_of,), jnp.float32, low / len(cuts), largest / len(cuts))
        level = level * jnp.repeat(jnp.exp(steps), dims[dim] // shards_of).reshape((-1,) + (1,) * (len(dims) - 1 - dim))
    return level


def bell_draw(rng, extent, width, bound, cuts=(), kind=jnp.bfloat16):
    values = jax.random.normal(rng, extent, jnp.float32) * width
    if len(cuts) > 0:
        values = levels(rng, extent, cuts, -0.22, 0.18) * values
    return jnp.clip(values, min=-bound, max=bound).astype(kind)


def setup_inputs(seed: int = 0) -> dict:
    seeds = jax.random.split(jax.random.key(seed), 10)
    flame_state = draw_flame_state(jax.random.fold_in(seeds[9], 71), 0)
    tangents = bell_draw(seeds[1], (DIRECTIONS, FIELDS, GRID_POINTS_ONE, CELLS), 1.0, 6.0, ((0, 4), (2, 64)), jnp.float32)
    direction_index = touch_ends(jax.random.randint(seeds[2], (DIRECTIONS,), 0, REACTIONS), jax.random.fold_in(seeds[2], 1), 0, REACTIONS - 1).astype(jnp.int32)
    reactant_table = draw_reactant_table(jax.random.fold_in(seeds[9], 71), 0)
    product_table = draw_product_table(jax.random.fold_in(seeds[9], 71), 0)
    natural_log_frequency = jnp.clip(jax.random.uniform(seeds[5], (REACTIONS,), jnp.float32, -3.0, -1.0), -3.0, -1.0)
    arrhenius_energy = jnp.clip(jnp.exp(jax.random.uniform(seeds[6], (REACTIONS,), jnp.float32, math.log(0.5), math.log(3.0))), 0.5, 3.0)
    diffusivity = jnp.clip(jnp.exp(jax.random.uniform(seeds[7], (FIELDS,), jnp.float32, math.log(0.03), math.log(0.25))), 0.03, 0.25)
    enthalpy = bell_draw(seeds[8], (SPECIES,), 0.1, 0.5, (), jnp.float32)
    return {"flame_state": flame_state, "tangents": tangents, "direction_index": direction_index, "reactant_table": reactant_table, "product_table": product_table, "natural_log_frequency": natural_log_frequency, "arrhenius_energy": arrhenius_energy, "diffusivity": diffusivity, "enthalpy": enthalpy}


time_step = 0.2
maximum_magnitude = lax.Precision.HIGHEST


def blockwise(kernel, arrays, block_cells):
    blocks = arrays[0].shape[-1] // block_cells

    def advance(block_id, results):
        offset = (block_id * block_cells).astype(jnp.int32)
        pieces = [lax.dynamic_slice_in_dim(operand_array, offset, block_cells, operand_array.ndim - 1) for operand_array in arrays]
        stored_numbers = kernel(*pieces)
        return tuple(lax.dynamic_update_slice_in_dim(result, value, offset, result.ndim - 1) for result, value in zip(results, stored_numbers))

    return lax.fori_loop(0, blocks, advance, tuple(jnp.zeros_like(operand_array) for operand_array in arrays))


def progress(stored_numbers, tables):
    consumed_multipliers, nu_net, natural_log_frequency, arrhenius_energy, enthalpy = tables
    exponent_numbers = stored_numbers[:-1]
    mixture_heat_level = stored_numbers[-1]
    exponent_speed = natural_log_frequency[:, None] - arrhenius_energy[:, None] / mixture_heat_level[None, :] + jnp.dot(consumed_multipliers, exponent_numbers, precision=maximum_magnitude)
    reaction_rates = jnp.exp(exponent_speed)
    production = jnp.dot(nu_net.T, reaction_rates, precision=maximum_magnitude)
    return reaction_rates, production


def nominal_chem(stored_numbers, tables):
    reaction_rates, production = progress(stored_numbers, tables)
    heat_term = -jnp.dot(tables[4], production, precision=maximum_magnitude)
    return (jnp.concatenate([production * jnp.exp(-stored_numbers[:-1]), heat_term[None, :]], 0),)


def joint_chem(stored_numbers, derivative_direction, selection_filter, tables):
    consumed_multipliers, nu_net, natural_log_frequency, arrhenius_energy, enthalpy = tables
    reaction_rates, production = progress(stored_numbers, tables)
    mixture_heat_level = stored_numbers[-1]
    inverse = jnp.exp(-stored_numbers[:-1])
    tangent_logs = derivative_direction[:, :-1]
    derivative_thermal_field = derivative_direction[:, -1]
    exponent_shift = selection_filter[:, :, None] + (arrhenius_energy[None, :, None] / (mixture_heat_level * mixture_heat_level)[None, None, :]) * derivative_thermal_field[:, None, :]
    exponent_shift = exponent_shift + jnp.einsum("rs,dsb->drb", consumed_multipliers, tangent_logs, precision=maximum_magnitude)
    production_change = jnp.einsum("rs,drb->dsb", nu_net, reaction_rates[None] * exponent_shift, precision=maximum_magnitude)
    heat_change = -jnp.einsum("s,dsb->db", enthalpy, production_change, precision=maximum_magnitude)
    heat_term = -jnp.dot(enthalpy, production, precision=maximum_magnitude)
    nominal = jnp.concatenate([production * inverse, heat_term[None, :]], 0)
    tangent_change = jnp.concatenate([(production_change - production[None] * tangent_logs) * inverse[None], heat_change[:, None, :]], 1)
    return nominal, tangent_change


def laplace(field_values, leading):
    summed = -6.0 * field_values
    for dimension in range(leading, leading + 3):
        summed = summed + jnp.roll(field_values, 1, dimension) + jnp.roll(field_values, -1, dimension)
    return summed


def reference(flame_state, tangents, direction_index, reactant_table, product_table, natural_log_frequency, arrhenius_energy, diffusivity, enthalpy):
    tables = (reactant_table.astype(jnp.float32), (product_table - reactant_table).astype(jnp.float32), natural_log_frequency, arrhenius_energy, enthalpy)
    fields = flame_state.shape[0]
    grid_state = flame_state.reshape(fields, GRID_POINTS_ONE, GRID_POINTS_TWO, GRID_POINTS_THREE)
    grid_tangents = tangents.reshape(tangents.shape[0], fields, GRID_POINTS_ONE, GRID_POINTS_TWO, GRID_POINTS_THREE)
    block_cells = GRID_POINTS_TWO * GRID_POINTS_THREE
    spread = diffusivity[:, None, None, None]

    def nominal_kernel(portion):
        return nominal_chem(portion, tables)

    def nominal_rate(stored_numbers):
        chemical = blockwise(nominal_kernel, (stored_numbers.reshape(fields, -1),), block_cells)[0]
        return chemical.reshape(stored_numbers.shape) + spread * laplace(stored_numbers, 1)

    start_rate = nominal_rate(grid_state)
    middle = grid_state + time_step * start_rate
    middle_rate = nominal_rate(middle)
    new_state = grid_state + 0.5 * time_step * (start_rate + middle_rate)
    reactions = reactant_table.shape[0]

    def advance_direction(element):
        derivative_direction, chosen = element
        selection_filter = (jnp.arange(reactions, dtype=jnp.int32) == chosen).astype(jnp.float32)[None, :]

        def joint_kernel(portion, tangent_portion):
            return joint_chem(portion, tangent_portion, selection_filter, tables)

        def tangent_rate(stored_numbers, field_values):
            combined = blockwise(joint_kernel, (stored_numbers.reshape(fields, -1), field_values.reshape(1, fields, -1)), block_cells)
            return combined[1].reshape(field_values.shape) + spread * laplace(field_values, 1)

        start_change = tangent_rate(grid_state, derivative_direction)
        middle_tangent = derivative_direction + time_step * start_change
        middle_change = tangent_rate(middle, middle_tangent)
        return derivative_direction + 0.5 * time_step * (start_change + middle_change)

    new_tangents = lax.map(advance_direction, (grid_tangents, direction_index))
    return new_state.reshape(flame_state.shape), new_tangents.reshape(tangents.shape)
```

```python
import jax
import jax.numpy as jnp
from jax import lax
from jax.experimental import pallas as pl
from jax.experimental.pallas import tpu as pltpu
from jax.sharding import Mesh
from jax.sharding import PartitionSpec as P

GRP = ("grp_0", "grp_1")
F = 54
FP = 56
RP = 336
TEMP = 53
f32 = jnp.float32
bf16 = jnp.bfloat16


def split(x):
    high = x.astype(bf16)
    return high, (x - high.astype(f32)).astype(bf16)


def rows_of(shape):
    return lax.broadcasted_iota(jnp.int32, shape, 0)


def exponents(x, weights, ones_from, ones_to):
    n = x.shape[1]
    high, low = split(jnp.concatenate([x, jnp.zeros((8, n), f32)], 0))
    row = rows_of((16, n))
    ones = jnp.where((row >= ones_from) & (row < ones_to), 1.0, 0.0)
    extra = jnp.where(row == 0, jnp.broadcast_to(x[TEMP : TEMP + 1, :], (16, n)), ones)
    rhs = jnp.concatenate([high, low, extra.astype(bf16)], 0)
    return jnp.dot(weights, rhs, preferred_element_type=f32)


def produced(rates, weights):
    high, low = split(rates)
    out = jnp.dot(weights, jnp.concatenate([high, low], 0), preferred_element_type=f32)
    last = out[48:56]
    heat = last + pltpu.roll(last, 7, 0) + pltpu.roll(last, 6, 0)
    row = rows_of(last.shape)
    last = jnp.where(row < 5, last, jnp.where(row == 5, heat, 0.0))
    return jnp.concatenate([out[:48], last], 0)


def with_last_row(x, value):
    last = jnp.where(rows_of((8, x.shape[1])) == 5, value, x[48:56])
    return jnp.concatenate([x[:48], last], 0)


def laplace(ref, p, j):
    c = ref[p, j]
    after = ref[p, (j + 1) & 3]
    before = ref[p, (j + 3) & 3]
    lane = lax.broadcasted_iota(jnp.int32, c.shape, 1)
    z = lane & 31
    total = pltpu.roll(jnp.where(lane >= 32, c, after), 96, 1)
    total = total + pltpu.roll(jnp.where(lane >= 96, before, c), 32, 1)
    total = total + jnp.where(z == 0, pltpu.roll(c, 97, 1), pltpu.roll(c, 1, 1))
    total = total + jnp.where(z == 31, pltpu.roll(c, 31, 1), pltpu.roll(c, 127, 1))
    return total + ref[p - 1, j] + ref[p + 1, j] - 6.0 * c


def near_kernel(place, own, even, odd, out):
    odd_side = place[0]
    pad = jnp.zeros((8, 512), f32)
    out[48:56, :] = pad
    sources = ((odd, 1 - odd_side), (own, odd_side), (own, 1 - odd_side), (even, odd_side))
    for p, (ref, start) in enumerate(sources):
        out[0:F, p * 128 : (p + 1) * 128] = ref[pl.ds(start, F, stride=2), :]


def nominal_section(x, w1, w2, rates_ref, aux_ref):
    n = x.shape[1]
    row = rows_of((8, n))
    temperature = jnp.broadcast_to(x[TEMP : TEMP + 1, :], (8, n))
    inverse_temperature = 1.0 / temperature
    rates = jnp.exp(exponents(with_last_row(x, -inverse_temperature), w1, 1, 4))
    rates_ref[...] = rates
    production = produced(rates, w2)
    inverse = jnp.exp(-x)
    last = jnp.where(row < 5, inverse[48:56], jnp.where(row == 5, 1.0, 0.0))
    inverse = jnp.concatenate([inverse[:48], last], 0)
    aux_ref[0:FP] = with_last_row(production, 0.0)
    aux_ref[FP : 2 * FP] = inverse
    aux_ref[2 * FP : 2 * FP + 8] = inverse_temperature * inverse_temperature
    return production * inverse


def nominal_kernel(place, own, core, other, other_core, even, odd, w1, w2, spread, rates_1, aux_1, rates_2, aux_2, out, state, slope, middle):
    odd_side = place[0]
    quarter = place[1]
    for blocks, k in ((own, 0), (core, 1), (other, 2), (other_core, 3)):
        for p in range(4):
            state[p + 1, quarter ^ k] = blocks[:, p * 128 : (p + 1) * 128]
    state[0, quarter, 48:56, :] = jnp.zeros((8, 128), f32)
    state[5, quarter, 48:56, :] = jnp.zeros((8, 128), f32)
    state[0, quarter, 0:F, :] = odd[pl.ds(odd_side, F, stride=2), :]
    state[5, quarter, 0:F, :] = even[pl.ds(1 - odd_side, F, stride=2), :]

    def first(step, carry):
        j = step >> 1
        half = step & 1
        p = 1 + 2 * half
        x = jnp.concatenate([state[p, j], state[p + 1, j]], 1)
        chem = nominal_section(x, w1[...], w2[...], rates_1.at[j, half], aux_1.at[j, half])
        slope[p, j] = chem[:, :128]
        slope[p + 1, j] = chem[:, 128:]
        return carry

    lax.fori_loop(0, 8, first, 0)

    def advance(p, j):
        s = slope[p, j] + spread[...] * laplace(state, p, j)
        slope[p, j] = s
        middle[p, j] = state[p, j] + 0.2 * s

    def diffuse(j, carry):
        advance(2, j)
        advance(3, j)
        return carry

    lax.fori_loop(0, 4, diffuse, 0)
    advance(1, quarter)
    advance(4, quarter)

    def second(j, carry):
        x = jnp.concatenate([middle[2, j], middle[3, j]], 1)
        chem = nominal_section(x, w1[...], w2[...], rates_2.at[j], aux_2.at[j])
        slope[2, j] = slope[2, j] + chem[:, :128]
        slope[3, j] = slope[3, j] + chem[:, 128:]
        return carry

    lax.fori_loop(0, 4, second, 0)
    for p, start in ((2, odd_side), (3, 1 - odd_side)):
        total = slope[p, quarter] + spread[...] * laplace(middle, p, quarter)
        new = state[p, quarter] + 0.1 * total
        out[pl.ds(start, F, stride=2), :] = new[0:F]


def tangent_section(u, w1, w2, rates, aux_ref):
    change_row = u[48:56] * aux_ref[2 * FP : 2 * FP + 8]
    change = exponents(with_last_row(u, change_row), w1, 4, 5)
    production_change = produced(rates * change, w2)
    return (production_change - aux_ref[0:FP] * u) * aux_ref[FP : 2 * FP]


def tangent_kernel(place, own, even, odd, rates_1, aux_1, rates_2, aux_2, w1, w2, spread, out, state, slope, middle):
    odd_side = place[0]
    sources = ((odd, odd_side), (odd, 1 - odd_side), (own, odd_side), (own, 1 - odd_side), (even, odd_side), (even, 1 - odd_side))
    for p, (ref, start) in enumerate(sources):
        for j in range(4):
            state[p, j, 48:56, :] = jnp.zeros((8, 128), f32)
            state[p, j, 0:F, :] = ref[pl.ds(start + 2 * j, F, stride=8), :]

    def first(step, carry):
        j = step >> 1
        half = step & 1
        p = 1 + 2 * half
        u = jnp.concatenate([state[p, j], state[p + 1, j]], 1)
        chem = tangent_section(u, w1[...], w2[...], rates_1[j, half], aux_1.at[j, half])
        slope[p, j] = chem[:, :128]
        slope[p + 1, j] = chem[:, 128:]
        return carry

    lax.fori_loop(0, 8, first, 0)

    def diffuse(j, carry):
        for p in range(1, 5):
            s = slope[p, j] + spread[...] * laplace(state, p, j)
            slope[p, j] = s
            middle[p, j] = state[p, j] + 0.2 * s
        return carry

    lax.fori_loop(0, 4, diffuse, 0)

    for j in range(4):
        u = jnp.concatenate([middle[2, j], middle[3, j]], 1)
        chem = tangent_section(u, w1[...], w2[...], rates_2[j], aux_2.at[j])
        for p, start in ((2, odd_side), (3, 1 - odd_side)):
            total = slope[p, j] + chem[:, (p - 2) * 128 : (p - 1) * 128] + spread[...] * laplace(middle, p, j)
            new = state[p, j] + 0.1 * total
            out[pl.ds(start + 2 * j, F, stride=8), :] = new[0:F]


def vmem(n):
    return [pl.BlockSpec(memory_space=pltpu.SMEM)] + [pl.BlockSpec(memory_space=pltpu.VMEM)] * n


def params():
    return pltpu.CompilerParams(vmem_limit_bytes=30 * 1024 * 1024)


def parts_of(x, count):
    parts = []
    for _ in range(count):
        part = lax.reduce_precision(x, 8, 7)
        parts.append(part)
        x = x - part
    return parts


def weights_of(reactant_table, product_table, log_frequency, energy, enthalpy, direction_index):
    reactions = reactant_table.shape[0]
    consumed = reactant_table.astype(f32)
    net = (product_table - reactant_table).astype(f32)
    high, low = parts_of(energy, 2)
    group = jnp.concatenate([consumed, high[:, None], jnp.zeros((reactions, 10), f32)], 1)
    extra = jnp.stack([low, *parts_of(log_frequency, 3)], 1)
    chosen = (jnp.arange(reactions, dtype=jnp.int32)[:, None] == direction_index[None, :]).astype(f32)
    first = []
    for d in range(direction_index.shape[0]):
        w = jnp.concatenate([group, group, extra, chosen[:, d : d + 1], jnp.zeros((reactions, 11), f32)], 1)
        first.append(jnp.pad(w, ((0, RP - reactions), (0, 0))).astype(bf16))
    heat = -jnp.sum(net * enthalpy[None, :], 1)
    rows = jnp.concatenate([net.T, jnp.stack(parts_of(heat, 3), 0), jnp.zeros((8, reactions), f32)], 0)
    rows = jnp.pad(rows, ((0, 0), (0, RP - reactions))).astype(bf16)
    return first, jnp.concatenate([rows, rows], 1)


def cell_rows(block):
    rows = block.reshape(*block.shape[:-1], 4, 128)
    return jnp.swapaxes(rows, -3, -2).reshape(-1, 128)


def shards(flame_state, tangents, direction_index, reactant_table, product_table, log_frequency, energy, diffusivity, enthalpy):
    count = lax.axis_size("sp")
    even = [(i, i ^ 1) for i in range(count)]
    odd = [(i, (i + 1 if i & 1 else i - 1) % count) for i in range(count)]
    swap = [(0, 1), (1, 0)]
    state_even = lax.ppermute(flame_state, "sp", even)
    state_odd = lax.ppermute(flame_state, "sp", odd)
    sides = []
    for d in range(3):
        sides.append((lax.ppermute(tangents[d], "sp", even), lax.ppermute(tangents[d], "sp", odd)))
    quarter = 2 * lax.axis_index("grp_0") + lax.axis_index("grp_1")
    place = jnp.stack([lax.axis_index("sp") & 1, quarter]).astype(jnp.int32)
    first, second = weights_of(reactant_table, product_table, log_frequency, energy, enthalpy, direction_index)
    spread = jnp.broadcast_to(jnp.pad(diffusivity, (0, FP - F))[:, None], (FP, 128))

    own_rows, even_rows, odd_rows = (x.reshape(2 * F, 128) for x in (flame_state, state_even, state_odd))
    near = pl.pallas_call(
        near_kernel,
        out_shape=jax.ShapeDtypeStruct((FP, 512), f32),
        in_specs=vmem(3),
        out_specs=pl.BlockSpec(memory_space=pltpu.VMEM),
        name="near_planes",
    )(place, own_rows, even_rows, odd_rows)
    other = lax.ppermute(near, "grp_0", swap)
    core = lax.ppermute(near, "grp_1", swap)
    other_core = lax.ppermute(other, "grp_1", swap)

    planes = pltpu.VMEM((6, 4, FP, 128), f32)
    aux_rows = 2 * FP + 8
    rates_1, aux_1, rates_2, aux_2, new_state = pl.pallas_call(
        nominal_kernel,
        out_shape=(
            jax.ShapeDtypeStruct((4, 2, RP, 256), f32),
            jax.ShapeDtypeStruct((4, 2, aux_rows, 256), f32),
            jax.ShapeDtypeStruct((4, RP, 256), f32),
            jax.ShapeDtypeStruct((4, aux_rows, 256), f32),
            jax.ShapeDtypeStruct((2 * F, 128), f32),
        ),
        in_specs=vmem(9),
        out_specs=tuple(pl.BlockSpec(memory_space=pltpu.VMEM) for _ in range(5)),
        scratch_shapes=[planes, planes, planes],
        compiler_params=params(),
        name="nominal",
    )(place, near, core, other, other_core, even_rows, odd_rows, first[0], second, spread)

    results = []
    for d in range(3):
        results.append(
            pl.pallas_call(
                tangent_kernel,
                out_shape=jax.ShapeDtypeStruct((8 * F, 128), f32),
                in_specs=vmem(10),
                out_specs=pl.BlockSpec(memory_space=pltpu.VMEM),
                scratch_shapes=[planes, planes, planes],
                compiler_params=params(),
                name="tangent",
            )(place, cell_rows(tangents[d]), cell_rows(sides[d][0]), cell_rows(sides[d][1]), rates_1, aux_1, rates_2, aux_2, first[d], second, spread)
        )
    rows = jnp.stack(results).reshape(3, F, 4, 2, 128)
    new_tangents = jnp.swapaxes(rows, 2, 3).reshape(tangents.shape)
    return new_state.reshape(flame_state.shape), new_tangents


def solution(mesh):
    split_mesh = Mesh(mesh.devices.reshape(2, 2, mesh.shape["sp"]), ("grp_0", "grp_1", "sp"))
    state = P(None, "sp", GRP)
    sensitivities = P(GRP, None, "sp", None)
    placed = (state, sensitivities, P(GRP), P(), P(), P(), P(), P(), P())
    return jax.shard_map(shards, mesh=split_mesh, in_specs=placed, out_specs=(state, sensitivities), check_vma=False)
```

```python
import functools

import jax
import jax.numpy as jnp
from jax import lax
from jax.experimental import pallas as pl
from jax.experimental.pallas import tpu as pltpu
from jax.sharding import Mesh
from jax.sharding import PartitionSpec as P

GRP = ("grp_0", "grp_1")
F = 54
FP = 56
RP = 336
TEMP = 53
f32 = jnp.float32
bf16 = jnp.bfloat16


def parts_of(x, count):
    parts = []
    for _ in range(count):
        part = x.astype(bf16).astype(f32)
        parts.append(part)
        x = x - part
    return parts


def rows_of(shape):
    return lax.broadcasted_iota(jnp.int32, shape, 0)


def exponents(x, weights, ones_from, ones_to):
    n = x.shape[1]
    row = rows_of((8, n))
    ones = jnp.where((row >= ones_from) & (row < ones_to), 1.0, 0.0)
    extra = jnp.where(row == 0, jnp.broadcast_to(x[TEMP : TEMP + 1, :], (8, n)), ones)
    high = jnp.concatenate([x, extra], 0).astype(bf16)
    low = (jnp.concatenate([x, extra], 0) - high.astype(f32)).astype(bf16)
    return jnp.dot(weights, jnp.concatenate([high, low], 0), preferred_element_type=f32)


def produced(rates, weights):
    high = rates.astype(bf16)
    low = (rates - high.astype(f32)).astype(bf16)
    out = jnp.dot(weights, high, preferred_element_type=f32) + jnp.dot(weights, low, preferred_element_type=f32)
    last = out[48:56]
    heat = last + pltpu.roll(last, 7, 0) + pltpu.roll(last, 6, 0)
    row = rows_of(last.shape)
    last = jnp.where(row < 5, last, jnp.where(row == 5, heat, 0.0))
    return jnp.concatenate([out[:48], last], 0)


def with_last_row(x, value):
    last = jnp.where(rows_of((8, x.shape[1])) == 5, value, x[48:56])
    return jnp.concatenate([x[:48], last], 0)


def laplace(ref, p, j):
    c = ref[p, j]
    after = ref[p, (j + 1) & 3]
    before = ref[p, (j + 3) & 3]
    lane = lax.broadcasted_iota(jnp.int32, c.shape, 1)
    z = lane & 31
    total = pltpu.roll(jnp.where(lane >= 32, c, after), 96, 1)
    total = total + pltpu.roll(jnp.where(lane >= 96, before, c), 32, 1)
    total = total + jnp.where(z == 0, pltpu.roll(c, 97, 1), pltpu.roll(c, 1, 1))
    total = total + jnp.where(z == 31, pltpu.roll(c, 31, 1), pltpu.roll(c, 127, 1))
    return total + ref[p - 1, j] + ref[p + 1, j] - 6.0 * c


def prepare_kernel(tangents, consumed, made, log_frequency, energy, diffusivity, enthalpy, chosen, t0, t1, t2, w1, w2, spread, sems):
    copies = [pltpu.make_async_copy(tangents.at[d], t, sems.at[d]) for d, t in enumerate((t0, t1, t2))]
    for copy in copies:
        copy.start()
    lanes = 384

    def wide(x):
        return jnp.pad(x, ((0, 0), (0, lanes - x.shape[1])))

    def row_of(ref):
        return wide(ref[...].reshape(1, ref.shape[0]))

    def placed(rows, shape):
        row = rows_of(shape)
        total = jnp.zeros(shape, f32)
        for k, value in rows.items():
            total = jnp.where(row == k, jnp.broadcast_to(value, shape), total)
        return total

    taken = wide(consumed[...].astype(f32))
    net = wide((made[...] - consumed[...]).astype(f32))
    high, low = parts_of(row_of(energy), 2)
    rows = {5: high, 8: low}
    for k, part in enumerate(parts_of(row_of(log_frequency), 3)):
        rows[9 + k] = part
    reaction = lax.broadcasted_iota(jnp.int32, (1, lanes), 1)
    for d in range(3):
        rows[12 + d] = (reaction == chosen[d]).astype(f32)
    zeros = jnp.zeros((11, lanes), f32)
    table = jnp.concatenate([taken, zeros], 0)
    table = jnp.concatenate([table[:48], table[48:64] + placed(rows, (16, lanes))], 0)
    w1[...] = jnp.concatenate([table, table], 0).T[:RP].astype(bf16)
    weighed = jnp.broadcast_to(jnp.pad(enthalpy[...].reshape(1, F - 1), ((0, 0), (0, 11))), (8, 64))
    table = jnp.concatenate([net, zeros], 0)
    heat = -jnp.dot(weighed, table, precision=lax.Precision.HIGHEST, preferred_element_type=f32)[:1]
    rows = {5 + k: part for k, part in enumerate(parts_of(heat, 3))}
    table = jnp.concatenate([table[:48], table[48:64] + placed(rows, (16, lanes))], 0)
    w2[...] = table[:, :RP].astype(bf16)
    spread[...] = jnp.broadcast_to(jnp.pad(diffusivity[...].reshape(1, F), ((0, 0), (0, 128 - F))), (128, 128)).T[:FP]
    for copy in copies:
        copy.wait()


def sides_of():
    return lax.axis_index("sp") & 1


def near_kernel(own, even, odd, out):
    odd_side = sides_of()
    out[48:56, :] = jnp.zeros((8, 512), f32)
    sources = ((odd, 1 - odd_side), (own, odd_side), (own, 1 - odd_side), (even, odd_side))
    for p, (ref, plane) in enumerate(sources):
        out[0:F, p * 128 : (p + 1) * 128] = ref[:, plane, :]


def nominal_section(x, w1, w2, rates_ref, aux_ref):
    n = x.shape[1]
    row = rows_of((8, n))
    temperature = jnp.broadcast_to(x[TEMP : TEMP + 1, :], (8, n))
    inverse_temperature = 1.0 / temperature
    rates = jnp.exp(exponents(with_last_row(x, -inverse_temperature), w1, 1, 4))
    rates_ref[...] = rates
    production = produced(rates, w2)
    inverse = jnp.exp(-x)
    last = jnp.where(row < 5, inverse[48:56], jnp.where(row == 5, 1.0, 0.0))
    inverse = jnp.concatenate([inverse[:48], last], 0)
    aux_ref[0:FP] = with_last_row(production, 0.0)
    aux_ref[FP : 2 * FP] = inverse
    aux_ref[2 * FP : 2 * FP + 8] = inverse_temperature * inverse_temperature
    return production * inverse


def planes_at(ref, first, last, j):
    return jnp.concatenate([ref[p, j] for p in range(first, last + 1)], 1)


def nominal_kernel(own, core, other, other_core, even, odd, w1, w2, spread, rates_1, aux_1, rates_2, aux_2, out, state, slope, middle):
    odd_side = sides_of()
    quarter = 2 * lax.axis_index("grp_0") + lax.axis_index("grp_1")
    for blocks, k in ((own, 0), (core, 1), (other, 2), (other_core, 3)):
        for p in range(4):
            state[p + 1, quarter ^ k] = blocks[:, p * 128 : (p + 1) * 128]
    state[0, quarter, 48:56, :] = jnp.zeros((8, 128), f32)
    state[5, quarter, 48:56, :] = jnp.zeros((8, 128), f32)
    state[0, quarter, 0:F, :] = odd[:, odd_side, :]
    state[5, quarter, 0:F, :] = even[:, 1 - odd_side, :]

    def first(j, carry):
        chem = nominal_section(planes_at(state, 1, 4, j), w1[...], w2[...], rates_1.at[j], aux_1.at[j])
        for p in range(4):
            slope[p + 1, j] = chem[:, p * 128 : (p + 1) * 128]
        return carry

    lax.fori_loop(0, 4, first, 0)

    def advance(p, j):
        s = slope[p, j] + spread[...] * laplace(state, p, j)
        slope[p, j] = s
        middle[p, j] = state[p, j] + 0.2 * s

    def diffuse(j, carry):
        advance(2, j)
        advance(3, j)
        return carry

    lax.fori_loop(0, 4, diffuse, 0)
    advance(1, quarter)
    advance(4, quarter)

    def second(j, carry):
        chem = nominal_section(planes_at(middle, 2, 3, j), w1[...], w2[...], rates_2.at[j], aux_2.at[j])
        slope[2, j] = slope[2, j] + chem[:, :128]
        slope[3, j] = slope[3, j] + chem[:, 128:]
        return carry

    lax.fori_loop(0, 4, second, 0)
    for p, plane in ((2, odd_side), (3, 1 - odd_side)):
        total = slope[p, quarter] + spread[...] * laplace(middle, p, quarter)
        new = state[p, quarter] + 0.1 * total
        out[:, plane, :] = new[0:F]


def tangent_section(u, w1, w2, rates_ref, aux_ref, d):
    change_row = u[48:56] * aux_ref[2 * FP : 2 * FP + 8]
    change = exponents(with_last_row(u, change_row), w1, 4 + d, 5 + d)
    production_change = produced(rates_ref[...] * change, w2)
    return (production_change - aux_ref[0:FP] * u) * aux_ref[FP : 2 * FP]


def tangent_kernel(own, even, odd, rates_1, aux_1, rates_2, aux_2, w1, w2, spread, *rest, d):
    out, result, state, slope, middle, sem = rest[-6:]
    odd_side = sides_of()
    sources = ((odd, odd_side), (odd, 1 - odd_side), (own, odd_side), (own, 1 - odd_side), (even, odd_side), (even, 1 - odd_side))
    for p, (ref, start) in enumerate(sources):
        for j in range(4):
            state[p, j, 48:56, :] = jnp.zeros((8, 128), f32)
            state[p, j, 0:F, :] = ref[pl.ds(start + 2 * j, F, stride=8), :]

    def first(j, carry):
        chem = tangent_section(planes_at(state, 1, 4, j), w1[...], w2[...], rates_1.at[j], aux_1.at[j], d)
        for p in range(4):
            slope[p + 1, j] = chem[:, p * 128 : (p + 1) * 128]
        return carry

    lax.fori_loop(0, 4, first, 0)

    def diffuse(j, carry):
        for p in range(1, 5):
            s = slope[p, j] + spread[...] * laplace(state, p, j)
            slope[p, j] = s
            middle[p, j] = state[p, j] + 0.2 * s
        return carry

    lax.fori_loop(0, 4, diffuse, 0)

    def second(j, carry):
        chem = tangent_section(planes_at(middle, 2, 3, j), w1[...], w2[...], rates_2.at[j], aux_2.at[j], d)
        for p, start in ((2, odd_side), (3, 1 - odd_side)):
            total = slope[p, j] + chem[:, (p - 2) * 128 : (p - 1) * 128] + spread[...] * laplace(middle, p, j)
            new = state[p, j] + 0.1 * total
            result[pl.ds(start + 2 * j, F, stride=8), :] = new[0:F]
        return carry

    lax.fori_loop(0, 4, second, 0)
    copy = pltpu.make_async_copy(result, out.at[pl.ds(d * 8 * F, 8 * F)], sem)
    copy.start()
    copy.wait()


VMEM = pl.BlockSpec(memory_space=pltpu.VMEM)
HBM = pl.BlockSpec(memory_space=pl.ANY)


def params(mebibytes):
    return pltpu.CompilerParams(vmem_limit_bytes=mebibytes * 1024 * 1024)


def cell_rows(block):
    rows = block.reshape(*block.shape[:-1], 4, 128)
    return jnp.swapaxes(rows, -3, -2).reshape(-1, 128)


def shards(flame_state, tangents, direction_index, reactant_table, product_table, log_frequency, energy, diffusivity, enthalpy):
    count = lax.axis_size("sp")
    even = [(i, i ^ 1) for i in range(count)]
    odd = [(i, (i + 1 if i & 1 else i - 1) % count) for i in range(count)]
    swap = [(0, 1), (1, 0)]
    state_even = lax.ppermute(flame_state, "sp", even)
    state_odd = lax.ppermute(flame_state, "sp", odd)
    *slices, w1, w2, spread = pl.pallas_call(
        prepare_kernel,
        out_shape=(
            *[jax.ShapeDtypeStruct(tangents.shape[1:], f32)] * 3,
            jax.ShapeDtypeStruct((RP, 128), bf16),
            jax.ShapeDtypeStruct((64, RP), bf16),
            jax.ShapeDtypeStruct((FP, 128), f32),
        ),
        in_specs=[HBM, *[VMEM] * 6, pl.BlockSpec(memory_space=pltpu.SMEM)],
        out_specs=(HBM, HBM, HBM, VMEM, VMEM, VMEM),
        scratch_shapes=[pltpu.SemaphoreType.DMA((3,))],
        compiler_params=params(4),
        name="prepare",
    )(tangents, reactant_table.T, product_table.T, log_frequency, energy, diffusivity, enthalpy, direction_index)
    sides = [(lax.ppermute(t, "sp", even), lax.ppermute(t, "sp", odd)) for t in slices]

    near = pl.pallas_call(
        near_kernel,
        out_shape=jax.ShapeDtypeStruct((FP, 512), f32),
        in_specs=[VMEM] * 3,
        out_specs=VMEM,
        compiler_params=params(2),
        name="near_planes",
    )(flame_state, state_even, state_odd)
    other = lax.ppermute(near, "grp_0", swap)
    core = lax.ppermute(near, "grp_1", swap)
    other_core = lax.ppermute(other, "grp_1", swap)

    planes = pltpu.VMEM((6, 4, FP, 128), f32)
    aux_rows = 2 * FP + 8
    rates_1, aux_1, rates_2, aux_2, new_state = pl.pallas_call(
        nominal_kernel,
        out_shape=(
            jax.ShapeDtypeStruct((4, RP, 512), f32),
            jax.ShapeDtypeStruct((4, aux_rows, 512), f32),
            jax.ShapeDtypeStruct((4, RP, 256), f32),
            jax.ShapeDtypeStruct((4, aux_rows, 256), f32),
            jax.ShapeDtypeStruct(flame_state.shape, f32),
        ),
        in_specs=[VMEM] * 9,
        out_specs=(VMEM,) * 5,
        scratch_shapes=[planes, planes, planes],
        compiler_params=params(10),
        name="nominal",
    )(near, core, other, other_core, state_even, state_odd, w1, w2, spread)

    rows = None
    for d in range(3):
        operands = [cell_rows(slices[d]), cell_rows(sides[d][0]), cell_rows(sides[d][1]), rates_1, aux_1, rates_2, aux_2, w1, w2, spread]
        if d:
            operands.append(rows)
        rows = pl.pallas_call(
            functools.partial(tangent_kernel, d=d),
            out_shape=jax.ShapeDtypeStruct((3 * 8 * F, 128), f32),
            in_specs=[VMEM] * 10 + [HBM] * (d > 0),
            out_specs=HBM,
            scratch_shapes=[pltpu.VMEM((8 * F, 128), f32), planes, planes, planes, pltpu.SemaphoreType.DMA],
            input_output_aliases={10: 0} if d else {},
            compiler_params=params(10),
            name="tangent",
        )(*operands)
    rows = rows.reshape(3, F, 4, 2, 128)
    return new_state, jnp.swapaxes(rows, 2, 3).reshape(tangents.shape)


def solution(mesh):
    split_mesh = Mesh(mesh.devices.reshape(2, 2, mesh.shape["sp"]), ("grp_0", "grp_1", "sp"))
    state = P(None, "sp", GRP)
    sensitivities = P(GRP, None, "sp", None)
    placed = (state, sensitivities, P(GRP), P(), P(), P(), P(), P(), P())
    return jax.shard_map(shards, mesh=split_mesh, in_specs=placed, out_specs=(state, sensitivities), check_vma=False)
```

```python
import jax
import jax.numpy as jnp
from jax import lax
from jax.experimental import pallas as pl
from jax.experimental.pallas import tpu as pltpu
from jax.sharding import Mesh
from jax.sharding import PartitionSpec as P

GRP = ("grp_0", "grp_1")
F = 54
FP = 56
RP = 336
TEMP = 53
f32 = jnp.float32
bf16 = jnp.bfloat16


def parts_of(x, count):
    parts = []
    for _ in range(count):
        part = x.astype(bf16).astype(f32)
        parts.append(part)
        x = x - part
    return parts


def rows_of(shape):
    return lax.broadcasted_iota(jnp.int32, shape, 0)


def exponents(x, weights, ones_from, ones_to):
    n = x.shape[1]
    row = rows_of((8, n))
    ones = jnp.where((row >= ones_from) & (row < ones_to), 1.0, 0.0)
    extra = jnp.where(row == 0, jnp.broadcast_to(x[TEMP : TEMP + 1, :], (8, n)), ones)
    high = jnp.concatenate([x, extra], 0).astype(bf16)
    low = (jnp.concatenate([x, extra], 0) - high.astype(f32)).astype(bf16)
    return jnp.dot(weights, jnp.concatenate([high, low], 0), preferred_element_type=f32)


def produced(rates, weights):
    high = rates.astype(bf16)
    low = (rates - high.astype(f32)).astype(bf16)
    out = jnp.dot(weights, high, preferred_element_type=f32) + jnp.dot(weights, low, preferred_element_type=f32)
    last = out[48:56]
    heat = last + pltpu.roll(last, 7, 0) + pltpu.roll(last, 6, 0)
    row = rows_of(last.shape)
    last = jnp.where(row < 5, last, jnp.where(row == 5, heat, 0.0))
    return jnp.concatenate([out[:48], last], 0)


def with_last_row(x, value):
    last = jnp.where(rows_of((8, x.shape[1])) == 5, value, x[48:56])
    return jnp.concatenate([x[:48], last], 0)


def laplace(ref, p, j):
    c = ref[p, j]
    after = ref[p, (j + 1) & 3]
    before = ref[p, (j + 3) & 3]
    lane = lax.broadcasted_iota(jnp.int32, c.shape, 1)
    z = lane & 31
    total = pltpu.roll(jnp.where(lane >= 32, c, after), 96, 1)
    total = total + pltpu.roll(jnp.where(lane >= 96, before, c), 32, 1)
    total = total + jnp.where(z == 0, pltpu.roll(c, 97, 1), pltpu.roll(c, 1, 1))
    total = total + jnp.where(z == 31, pltpu.roll(c, 31, 1), pltpu.roll(c, 127, 1))
    return total + ref[p - 1, j] + ref[p + 1, j] - 6.0 * c


def prepare_kernel(tangents, consumed_in, made_in, log_frequency_in, energy_in, diffusivity_in, enthalpy_in, chosen, own, w1, w2, spread, *scratch):
    consumed, made, log_frequency, energy, diffusivity, enthalpy, sems = scratch
    sources = (consumed_in, made_in, log_frequency_in, energy_in, diffusivity_in, enthalpy_in, tangents)
    copies = [pltpu.make_async_copy(source, target, sems.at[k]) for k, (source, target) in enumerate(zip(sources, (*scratch[:-1], own)))]
    for copy in copies:
        copy.start()
    for copy in copies[:-1]:
        copy.wait()
    lanes = 384

    def wide(x):
        return jnp.pad(x, ((0, 0), (0, lanes - x.shape[1])))

    def row_of(ref):
        return wide(ref[...].reshape(1, ref.shape[0]))

    def placed(rows, shape):
        row = rows_of(shape)
        total = jnp.zeros(shape, f32)
        for k, value in rows.items():
            total = jnp.where(row == k, jnp.broadcast_to(value, shape), total)
        return total

    taken = wide(consumed[...].astype(f32))
    net = wide((made[...] - consumed[...]).astype(f32))
    high, low = parts_of(row_of(energy), 2)
    rows = {5: high, 8: low}
    for k, part in enumerate(parts_of(row_of(log_frequency), 3)):
        rows[9 + k] = part
    reaction = lax.broadcasted_iota(jnp.int32, (1, lanes), 1)
    for d in range(3):
        rows[12 + d] = (reaction == chosen[d]).astype(f32)
    zeros = jnp.zeros((11, lanes), f32)
    table = jnp.concatenate([taken, zeros], 0)
    table = jnp.concatenate([table[:48], table[48:64] + placed(rows, (16, lanes))], 0)
    w1[...] = jnp.concatenate([table, table], 0).T[:RP].astype(bf16)
    weighed = jnp.broadcast_to(jnp.pad(enthalpy[...].reshape(1, F - 1), ((0, 0), (0, 11))), (8, 64))
    table = jnp.concatenate([net, zeros], 0)
    heat = -jnp.dot(weighed, table, precision=lax.Precision.HIGHEST, preferred_element_type=f32)[:1]
    rows = {5 + k: part for k, part in enumerate(parts_of(heat, 3))}
    table = jnp.concatenate([table[:48], table[48:64] + placed(rows, (16, lanes))], 0)
    w2[...] = table[:, :RP].astype(bf16)
    spread[...] = jnp.broadcast_to(jnp.pad(diffusivity[...].reshape(1, F), ((0, 0), (0, 128 - F))), (128, 128)).T[:FP]
    copies[-1].wait()


def sides_of():
    return lax.axis_index("sp") & 1


def near_kernel(own, even, odd, out):
    odd_side = sides_of()
    out[48:56, :] = jnp.zeros((8, 512), f32)
    sources = ((odd, 1 - odd_side), (own, odd_side), (own, 1 - odd_side), (even, odd_side))
    for p, (ref, plane) in enumerate(sources):
        out[0:F, p * 128 : (p + 1) * 128] = ref[:, plane, :]


def nominal_section(x, w1, w2, rates_ref, aux_ref):
    n = x.shape[1]
    row = rows_of((8, n))
    temperature = jnp.broadcast_to(x[TEMP : TEMP + 1, :], (8, n))
    inverse_temperature = 1.0 / temperature
    rates = jnp.exp(exponents(with_last_row(x, -inverse_temperature), w1, 1, 4))
    rates_ref[...] = rates
    production = produced(rates, w2)
    inverse = jnp.exp(-x)
    last = jnp.where(row < 5, inverse[48:56], jnp.where(row == 5, 1.0, 0.0))
    inverse = jnp.concatenate([inverse[:48], last], 0)
    aux_ref[0:FP] = with_last_row(production, 0.0)
    aux_ref[FP : 2 * FP] = inverse
    aux_ref[2 * FP : 2 * FP + 8] = inverse_temperature * inverse_temperature
    return production * inverse


def planes_at(ref, first, last, j):
    return jnp.concatenate([ref[p, j] for p in range(first, last + 1)], 1)


def nominal_kernel(own, core, other, other_core, even, odd, w1, w2, spread, rates_1, aux_1, rates_2, aux_2, out, state, slope, middle):
    odd_side = sides_of()
    quarter = 2 * lax.axis_index("grp_0") + lax.axis_index("grp_1")
    for blocks, k in ((own, 0), (core, 1), (other, 2), (other_core, 3)):
        for p in range(4):
            state[p + 1, quarter ^ k] = blocks[:, p * 128 : (p + 1) * 128]
    state[0, quarter, 48:56, :] = jnp.zeros((8, 128), f32)
    state[5, quarter, 48:56, :] = jnp.zeros((8, 128), f32)
    state[0, quarter, 0:F, :] = odd[:, odd_side, :]
    state[5, quarter, 0:F, :] = even[:, 1 - odd_side, :]

    def first(j, carry):
        chem = nominal_section(planes_at(state, 1, 4, j), w1[...], w2[...], rates_1.at[j], aux_1.at[j])
        for p in range(4):
            slope[p + 1, j] = chem[:, p * 128 : (p + 1) * 128]
        return carry

    lax.fori_loop(0, 4, first, 0, unroll=UNROLL)

    def advance(p, j):
        s = slope[p, j] + spread[...] * laplace(state, p, j)
        slope[p, j] = s
        middle[p, j] = state[p, j] + 0.2 * s

    def diffuse(j, carry):
        advance(2, j)
        advance(3, j)
        return carry

    lax.fori_loop(0, 4, diffuse, 0)
    advance(1, quarter)
    advance(4, quarter)

    def second(j, carry):
        chem = nominal_section(planes_at(middle, 2, 3, j), w1[...], w2[...], rates_2.at[j], aux_2.at[j])
        slope[2, j] = slope[2, j] + chem[:, :128]
        slope[3, j] = slope[3, j] + chem[:, 128:]
        return carry

    lax.fori_loop(0, 4, second, 0, unroll=UNROLL)
    for p, plane in ((2, odd_side), (3, 1 - odd_side)):
        total = slope[p, quarter] + spread[...] * laplace(middle, p, quarter)
        new = state[p, quarter] + 0.1 * total
        out[:, plane, :] = new[0:F]


def tangent_section(u, w1, w2, rates_ref, aux_ref, d):
    change_row = u[48:56] * aux_ref[2 * FP : 2 * FP + 8]
    change = exponents(with_last_row(u, change_row), w1, 4 + d, 5 + d)
    production_change = produced(rates_ref[...] * change, w2)
    return (production_change - aux_ref[0:FP] * u) * aux_ref[FP : 2 * FP]


def tangent_kernel(own, even, odd, rates_1, aux_1, rates_2, aux_2, w1, w2, spread, out, result, state, slope, middle, sems):
    odd_side = sides_of()
    sources = ((odd, odd_side), (odd, 1 - odd_side), (own, odd_side), (own, 1 - odd_side), (even, odd_side), (even, 1 - odd_side))
    rows = 8 * F

    def written(d):
        return pltpu.make_async_copy(result.at[d], out.at[pl.ds(d * rows, rows)], sems.at[d])

    def direction(d, carry):
        for p, (ref, start) in enumerate(sources):
            for j in range(4):
                state[p, j, 48:56, :] = jnp.zeros((8, 128), f32)
                state[p, j, 0:F, :] = ref[pl.ds(d * rows + start + 2 * j, F, stride=8), :]

        def first(j, carry):
            chem = tangent_section(planes_at(state, 1, 4, j), w1[...], w2[...], rates_1.at[j], aux_1.at[j], d)
            for p in range(4):
                slope[p + 1, j] = chem[:, p * 128 : (p + 1) * 128]
            return carry

        lax.fori_loop(0, 4, first, 0, unroll=UNROLL)

        def diffuse(j, carry):
            for p in range(1, 5):
                s = slope[p, j] + spread[...] * laplace(state, p, j)
                slope[p, j] = s
                middle[p, j] = state[p, j] + 0.2 * s
            return carry

        lax.fori_loop(0, 4, diffuse, 0)

        def second(j, carry):
            chem = tangent_section(planes_at(middle, 2, 3, j), w1[...], w2[...], rates_2.at[j], aux_2.at[j], d)
            for p, start in ((2, odd_side), (3, 1 - odd_side)):
                total = slope[p, j] + chem[:, (p - 2) * 128 : (p - 1) * 128] + spread[...] * laplace(middle, p, j)
                new = state[p, j] + 0.1 * total
                result[d, pl.ds(start + 2 * j, F, stride=8), :] = new[0:F]
            return carry

        lax.fori_loop(0, 4, second, 0, unroll=UNROLL)
        written(d).start()
        return carry

    lax.fori_loop(0, 3, direction, 0)
    for d in range(3):
        written(d).wait()


UNROLL = 2
VMEM = pl.BlockSpec(memory_space=pltpu.VMEM)
HBM = pl.BlockSpec(memory_space=pltpu.HBM)


def params(mebibytes):
    return pltpu.CompilerParams(vmem_limit_bytes=mebibytes * 1024 * 1024)


def cell_rows(block):
    rows = block.reshape(*block.shape[:-1], 4, 128)
    return jnp.swapaxes(rows, -3, -2).reshape(-1, 128)


def shards(flame_state, tangents, direction_index, reactant_table, product_table, log_frequency, energy, diffusivity, enthalpy):
    count = lax.axis_size("sp")
    even = [(i, i ^ 1) for i in range(count)]
    odd = [(i, (i + 1 if i & 1 else i - 1) % count) for i in range(count)]
    swap = [(0, 1), (1, 0)]
    state_odd = lax.ppermute(flame_state, "sp", odd)
    tangents_odd = lax.ppermute(tangents, "sp", odd)
    state_even = lax.ppermute(flame_state, "sp", even)
    tangents_even = lax.ppermute(tangents, "sp", even)
    tables = (tangents, reactant_table.T, product_table.T, log_frequency, energy, diffusivity, enthalpy)
    own, w1, w2, spread = pl.pallas_call(
        prepare_kernel,
        out_shape=(
            jax.ShapeDtypeStruct(tangents.shape, f32),
            jax.ShapeDtypeStruct((RP, 128), bf16),
            jax.ShapeDtypeStruct((64, RP), bf16),
            jax.ShapeDtypeStruct((FP, 128), f32),
        ),
        in_specs=[HBM] * 7 + [pl.BlockSpec(memory_space=pltpu.SMEM)],
        out_specs=(VMEM,) * 4,
        scratch_shapes=[
            *[pltpu.VMEM((F - 1, reactant_table.shape[0]), jnp.int32)] * 2,
            *[pltpu.VMEM(x.shape, f32) for x in (log_frequency, energy, diffusivity, enthalpy)],
            pltpu.SemaphoreType.DMA((7,)),
        ],
        compiler_params=params(4),
        name="prepare",
    )(*[pltpu.with_memory_space_constraint(x, pltpu.HBM) for x in tables], direction_index)

    near = pl.pallas_call(
        near_kernel,
        out_shape=jax.ShapeDtypeStruct((FP, 512), f32),
        in_specs=[VMEM] * 3,
        out_specs=VMEM,
        compiler_params=params(2),
        name="near_planes",
    )(flame_state, state_even, state_odd)
    other = lax.ppermute(near, "grp_0", swap)
    core = lax.ppermute(near, "grp_1", swap)
    other_core = lax.ppermute(other, "grp_1", swap)

    planes = pltpu.VMEM((6, 4, FP, 128), f32)
    aux_rows = 2 * FP + 8
    rates_1, aux_1, rates_2, aux_2, new_state = pl.pallas_call(
        nominal_kernel,
        out_shape=(
            jax.ShapeDtypeStruct((4, RP, 512), f32),
            jax.ShapeDtypeStruct((4, aux_rows, 512), f32),
            jax.ShapeDtypeStruct((4, RP, 256), f32),
            jax.ShapeDtypeStruct((4, aux_rows, 256), f32),
            jax.ShapeDtypeStruct(flame_state.shape, f32),
        ),
        in_specs=[VMEM] * 9,
        out_specs=(VMEM,) * 5,
        scratch_shapes=[planes, planes, planes],
        compiler_params=params(10),
        name="nominal",
    )(near, core, other, other_core, state_even, state_odd, w1, w2, spread)

    rows = pl.pallas_call(
        tangent_kernel,
        out_shape=jax.ShapeDtypeStruct((3 * 8 * F, 128), f32),
        in_specs=[VMEM] * 10,
        out_specs=HBM,
        scratch_shapes=[pltpu.VMEM((3, 8 * F, 128), f32), planes, planes, planes, pltpu.SemaphoreType.DMA((3,))],
        compiler_params=params(10),
        name="tangent",
    )(cell_rows(own), cell_rows(tangents_even), cell_rows(tangents_odd), rates_1, aux_1, rates_2, aux_2, w1, w2, spread)
    rows = rows.reshape(3, F, 4, 2, 128)
    return new_state, jnp.swapaxes(rows, 2, 3).reshape(tangents.shape)


def solution(mesh):
    split_mesh = Mesh(mesh.devices.reshape(2, 2, mesh.shape["sp"]), ("grp_0", "grp_1", "sp"))
    state = P(None, "sp", GRP)
    sensitivities = P(GRP, None, "sp", None)
    placed = (state, sensitivities, P(GRP), P(), P(), P(), P(), P(), P())


    return jax.shard_map(shards, mesh=split_mesh, in_specs=placed, out_specs=(state, sensitivities), check_vma=False)
```
